32 devices in a mesh: genome: 8 (over z, x), samples: 4 (over y, core).
Axes of the slice: x: 2, y: 2, z: 4, core: 2. Of those that a mesh axis runs over, the one named last changes fastest.
Arguments:
- genotypes: int32 [4096, 12288], P('samples', 'genome'), may hold values from 0 to 2
- residuals: bfloat16 [4096, 64], P('samples'), may hold values from -78 to 78
- variant_class: int32 [12288], P('genome'), may hold values from 0 to 7
- class_weight: float32 [8], replicated, may hold values from 0.25 to 4
- gene_start: int32 [512], P(('genome', 'samples')), may hold values from 0 to 12287, as said below
- gene_end: int32 [512], P(('genome', 'samples')), may hold values from 1 to 12288, as said below
Outputs:
- score_track: float32 [12288, 64], P(('genome', 'samples'))
- gene_stat: float32 [512, 64], P(('genome', 'samples'))
The draws below stay inside these ranges and needn't reach their ends.
Inputs may be any that keep to these rules, and one draw needn't show every extreme that they name: gene_end[g] - 1 lies in [k * 384, (k + 1) * 384) with k = g // 16. 1 <= gene_end[g] - gene_start[g] <= 384.
All inputs are finite; a program needn't handle non-finite values.
Results may differ from the reference program's by a relative error of at most 0.0003.
Values sent between devices are 32-bit elements; how exact they have to be, the bound alone decides.
A program may use at most 64 MiB of HBM per device.

```python
import math
import jax
import jax.numpy as jnp
from jax import lax

PHENO = 64
CLASSES = 8
S_DEV = 1024
GENE_DEV = 16
SAMPLES = 4096
VARIANTS = 12288
GENES = 512
N_SAMPLES = 4


def log_uniform(key, shape, lower, upper):
    return jnp.exp(jax.random.uniform(key, shape, jnp.float32, math.log(lower), math.log(upper)))


def draw_genotypes(key, part):
    key_rate, key_first, key_second = jax.random.split(jax.random.fold_in(key, 11), 3)
    base_rate = jax.random.randint(key_rate, (VARIANTS,), 1, 8)
    rising = 7 * jnp.arange(VARIANTS, dtype=jnp.int32) // VARIANTS
    allele_rate = (base_rate + rising)[None, :]
    first_draw = jax.random.randint(key_first, (SAMPLES, VARIANTS), 0, 16)
    second_draw = jax.random.randint(key_second, (SAMPLES, VARIANTS), 0, 16)
    return ((first_draw < allele_rate).astype(jnp.int32) + (second_draw < allele_rate).astype(jnp.int32)).astype(jnp.int32)


def draw_residuals(key, part):
    key_noise, key_rows, key_cols = jax.random.split(jax.random.fold_in(key, 23), 3)
    position = jnp.arange(SAMPLES, dtype=jnp.float32) / SAMPLES
    trend = jnp.sqrt(1.0 + 2.0 * position)
    noise = jnp.clip(jax.random.normal(key_noise, (SAMPLES, PHENO), jnp.float32), -5.0, 5.0)
    row_scale = log_uniform(key_rows, (SAMPLES,), 0.3, 3.0) * trend
    col_scale = log_uniform(key_cols, (PHENO,), 0.3, 3.0)
    return (noise * row_scale[:, None] * col_scale[None, :]).astype(jnp.bfloat16)


def gene_bounds(key):
    key_last, key_length = jax.random.split(jax.random.fold_in(key, 37), 2)
    genes_index = jnp.arange(GENES, dtype=jnp.int32)
    block_index = genes_index // GENE_DEV
    block_size = VARIANTS // (GENES // GENE_DEV)
    last_variant = block_index * block_size + jax.random.randint(key_last, (GENES,), 0, block_size)
    window_length = jax.random.randint(key_length, (GENES,), 1, block_size + 1)
    end_index = last_variant + 1
    start_index = jnp.maximum(end_index - window_length, 0)
    return (start_index.astype(jnp.int32), end_index.astype(jnp.int32))


def draw_gene_start(key, part):
    return gene_bounds(key)[0]


def draw_gene_end(key, part):
    return gene_bounds(key)[1]


def place_ends(drawn, stream_key, low, top_value):
    longest = drawn.shape.index(max(drawn.shape))
    spots = []
    for shift in (0, 1):
        where = [jax.random.randint(jax.random.fold_in(stream_key, axis), (), 0, length) for axis, length in enumerate(drawn.shape)]
        where[longest] = (where[longest] + shift) % drawn.shape[longest]
        spots.append(tuple(where))
    return drawn.at[spots[0]].set(low).at[spots[1]].set(top_value)


def setup_inputs(seed: int = 0) -> dict:
    key_list = jax.random.split(jax.random.key(seed), 7)
    genotypes = draw_genotypes(jax.random.fold_in(key_list[6], 71), 0)
    residuals = draw_residuals(jax.random.fold_in(key_list[6], 71), 0)
    variant_class = place_ends(jax.random.randint(key_list[2], (VARIANTS,), 0, CLASSES), jax.random.fold_in(key_list[2], 1), 0, CLASSES - 1).astype(jnp.int32)
    class_weight = jnp.clip(jnp.exp(jax.random.uniform(key_list[3], (CLASSES,), jnp.float32, math.log(0.25), math.log(4.0))), 0.25, 4.0)
    gene_start = draw_gene_start(jax.random.fold_in(key_list[6], 71), 0)
    gene_end = draw_gene_end(jax.random.fold_in(key_list[6], 71), 0)
    return dict(genotypes=genotypes, residuals=residuals, variant_class=variant_class, class_weight=class_weight, gene_start=gene_start, gene_end=gene_end)


def reference(genotypes, residuals, variant_class, class_weight, gene_start, gene_end):
    contract = (((0,), (0,)), ((), ()))

    def add_block(block_index, carry):
        partial_value, squared = carry
        offset = (block_index * S_DEV).astype(jnp.int32)
        sample_block = lax.dynamic_slice_in_dim(genotypes, offset, S_DEV, 0).astype(jnp.bfloat16)
        residual_block = lax.dynamic_slice_in_dim(residuals, offset, S_DEV, 0)
        partial_value = partial_value + lax.dot_general(sample_block, residual_block, contract, preferred_element_type=jnp.float32)
        squared = squared + lax.dot_general(sample_block * sample_block, jnp.ones((S_DEV,), jnp.bfloat16), contract, preferred_element_type=jnp.float32)
        return (partial_value, squared)

    start_sums = (jnp.zeros((VARIANTS, PHENO), jnp.float32), jnp.zeros((VARIANTS,), jnp.float32))
    partial_value, counts = lax.fori_loop(0, N_SAMPLES, add_block, start_sums)
    weight = class_weight[variant_class]
    scores = partial_value * weight[:, None] * (SAMPLES ** -0.5)
    quad_terms = weight * weight * counts / SAMPLES
    spread = jnp.sum(jnp.square(residuals.astype(jnp.float32)), axis=0) / SAMPLES + 1e-5
    prefix = jnp.cumsum(scores, axis=0)
    quad_prefix = jnp.cumsum(quad_terms)
    score_track = prefix * (VARIANTS ** -0.5)
    padded = jnp.concatenate([jnp.zeros((1, PHENO), jnp.float32), prefix], axis=0)
    quad_padded = jnp.concatenate([jnp.zeros((1,), jnp.float32), quad_prefix], axis=0)
    gene_score = padded[gene_end] - padded[gene_start]
    gene_quad = quad_padded[gene_end] - quad_padded[gene_start]
    gene_stat = jnp.square(gene_score) / (spread[None, :] * (gene_quad[:, None] + 1.0))
    return (score_track, gene_stat)
```

```python
import functools

import jax
import jax.numpy as jnp
from jax import lax
from jax.experimental import pallas as pl
from jax.experimental.pallas import tpu as pltpu
from jax.sharding import PartitionSpec as P

MESH = pl.DeviceIdType.MESH
GROUPS = 4
LANES = 128
VMEM_LIMIT = 24 * 1024 * 1024


def prefix(x, axis, combine, identity):
    peers, place = (lax.axis_size(axis), lax.axis_index(axis))
    everything = jax.tree.map(lambda part: lax.all_gather(part, axis), x)
    start = jax.tree.map(
        lambda part, zero: jnp.broadcast_to(jnp.asarray(zero, part.dtype), part.shape), x, identity
    )

    def step(k, before):
        reached = k < place
        new = combine(before, jax.tree.map(lambda part: part[k], everything))
        return jax.tree.map(lambda a, b: jnp.where(reached, a, b), new, before)

    return lax.fori_loop(0, peers, step, start)


def passed_along(value, axis, steps):
    count = lax.axis_size(axis)
    leading, last = (max(0, -steps), min(count, count - steps))
    return lax.ppermute(value, axis, [(source, source + steps) for source in range(leading, last)])


def add_pairs(earlier, later):
    return (earlier[0] + later[0], earlier[1] + later[1])


def prefix_rows(values):
    rows, columns = values.shape
    block_width = 128
    block_count = rows // block_width
    positions = jnp.arange(block_width)
    lower_ones = (positions[:, None] >= positions[None, :]).astype(jnp.float32)
    blocks = values.reshape(block_count, block_width, columns)
    inner_sums = jnp.einsum("ij,bjk->bik", lower_ones, blocks, precision=lax.Precision.HIGHEST)
    totals = inner_sums[:, -1, :]
    before = jnp.cumsum(totals, axis=0) - totals
    return (inner_sums + before[:, None, :]).reshape(rows, columns)


def local(genotypes, residuals, variant_class, class_weight, gene_start, gene_end):
    groups = lax.axis_size("samples")
    genome_count = lax.axis_size("genome")
    sample_rows, block_vars = genotypes.shape
    phenos = residuals.shape[1]
    share_rows = block_vars // groups
    total_samples = sample_rows * groups
    total_vars = block_vars * genome_count
    sample_part = lax.axis_index("samples")
    flat_index = lax.axis_index("genome") * groups + sample_part
    contract = (((0,), (0,)), ((), ()))
    dosage = genotypes.astype(jnp.bfloat16)
    partial_value = lax.dot_general(dosage, residuals, contract, preferred_element_type=jnp.float32)
    squared = lax.dot_general(
        dosage * dosage,
        jnp.ones((sample_rows,), jnp.bfloat16),
        contract,
        preferred_element_type=jnp.float32,
    )
    spread_local = jnp.sum(jnp.square(residuals.astype(jnp.float32)), axis=0)
    carry_zero = (jnp.zeros((phenos,), jnp.float32), jnp.zeros((), jnp.float32))
    summed, counts, spread_sum = lax.psum((partial_value, squared, spread_local), "samples")
    classes = jnp.arange(class_weight.shape[0], dtype=jnp.int32)
    weight = jnp.sum(
        jnp.where(variant_class[:, None] == classes[None, :], class_weight[None, :], 0.0), axis=1
    )
    scores = summed * weight[:, None] * total_samples ** (-0.5)
    quad_terms = weight * weight * counts / total_samples
    local_prefix = prefix_rows(scores)
    local_quad = prefix_rows(quad_terms[:, None])[:, 0]
    ends = (local_prefix[-1], local_quad[-1])
    carry_sum, carry_quad = prefix(ends, "genome", add_pairs, carry_zero)
    full_prefix = local_prefix + carry_sum[None, :]
    source, quad_source = (local_prefix, local_quad)
    last_rows = source[block_vars - share_rows :]
    last_quad = quad_source[block_vars - share_rows :]
    incoming, incoming_quad = passed_along((last_rows, last_quad), "genome", 1)
    incoming = incoming - incoming[-1][None, :]
    incoming_quad = incoming_quad - incoming_quad[-1]
    near_start = jnp.maximum(sample_part - 1, 0) * share_rows
    own_start = sample_part * share_rows
    near_rows = lax.dynamic_slice_in_dim(source, near_start, share_rows, 0)
    near_quad = lax.dynamic_slice_in_dim(quad_source, near_start, share_rows, 0)
    at_first = sample_part == 0
    prior_rows = jnp.where(at_first, incoming, near_rows)
    prior_quad = jnp.where(at_first, incoming_quad, near_quad)
    own_rows = lax.dynamic_slice_in_dim(source, own_start, share_rows, 0)
    own_quad = lax.dynamic_slice_in_dim(quad_source, own_start, share_rows, 0)
    track_rows = lax.dynamic_slice_in_dim(full_prefix, own_start, share_rows, 0)
    window = jnp.concatenate([prior_rows, own_rows], axis=0)
    quad_window = jnp.concatenate([prior_quad, own_quad], axis=0)
    window_base = (flat_index - 1) * share_rows
    positions = jnp.arange(2 * share_rows, dtype=jnp.int32)
    end_pos = gene_end - 1 - window_base
    start_pos = gene_start - 1 - window_base
    picker = (positions[None, :] == end_pos[:, None]).astype(jnp.float32) - (
        positions[None, :] == start_pos[:, None]
    ).astype(jnp.float32)
    gene_score = jnp.dot(
        picker, window, precision=lax.Precision.HIGHEST, preferred_element_type=jnp.float32
    )
    gene_quad = jnp.dot(
        picker, quad_window, precision=lax.Precision.HIGHEST, preferred_element_type=jnp.float32
    )
    variance = spread_sum / total_samples + 1e-05
    gene_stat = jnp.square(gene_score) / (variance[None, :] * (gene_quad[:, None] + 1.0))
    return (track_rows * total_vars ** (-0.5), gene_stat)


def split3(x):
    high = x.astype(jnp.bfloat16)
    rest = x - high.astype(jnp.float32)
    mid = rest.astype(jnp.bfloat16)
    low = (rest - mid.astype(jnp.float32)).astype(jnp.bfloat16)
    return jnp.concatenate([high, mid, low], axis=0)


def dot3(x, y):
    rows = x.shape[0]
    out = jnp.dot(split3(x), y, preferred_element_type=jnp.float32)
    return out[:rows] + out[rows : 2 * rows] + out[2 * rows :]


def kernel(
    genome_count, geno_hbm, res_hbm, class_hbm, cw_hbm, start_hbm, end_hbm,
    track_ref, stat_ref,
    res_ref, class_ref, cw_ref, bounds_ref, small_sem,
    geno, scores, relay, partials, bounds_in, gene_out, gene_in, tot_out, tot_in,
    geno_sem, rs_send, rs_recv, bd_send, bd_recv, bn_send, bn_recv,
    ge_send, ge_recv, gn_send, gn_recv, to_send, to_recv,
):
    g = lax.axis_index("genome")
    s = lax.axis_index("samples")
    sample_rows, share = geno.shape[1:]
    block = share * GROUPS
    phenos = res_ref.shape[0]
    genes = stat_ref.shape[0]
    depth = scores.shape[1]
    total_samples = sample_rows * GROUPS
    peers = [lax.rem(s + 2, 4), 3 - s, s + 1 - 2 * lax.rem(s, 2)]
    owners = peers + [s]

    smalls = []
    for i, (src, dst) in enumerate([
        (res_hbm, res_ref), (class_hbm, class_ref), (cw_hbm, cw_ref),
        (start_hbm, bounds_ref.at[0]), (end_hbm, bounds_ref.at[1]),
    ]):
        copy = pltpu.make_async_copy(src, dst, small_sem.at[i])
        copy.start()
        smalls.append(copy)
    loads = []
    for j, owner in enumerate(owners):
        columns = pl.ds(pl.multiple_of(owner * share, LANES), share)
        copy = pltpu.make_async_copy(geno_hbm.at[:, columns], geno.at[j], geno_sem.at[j])
        copy.start()
        loads.append(copy)

    barrier = pltpu.get_barrier_semaphore()
    for dg in range(genome_count):
        for ds in range(GROUPS):
            if dg or ds:
                there = (lax.rem(g + dg, genome_count), lax.rem(s + ds, GROUPS))
                pl.semaphore_signal(barrier, inc=1, device_id=there, device_id_type=MESH)

    def remote(src, dst, send, recv, there):
        return pltpu.make_async_remote_copy(
            src_ref=src, dst_ref=dst, send_sem=send, recv_sem=recv,
            device_id=there, device_id_type=MESH,
        )

    def chunk(j):
        loads[j].wait()
        acc = jnp.zeros((phenos, share), jnp.float32)
        squares = jnp.zeros((8, share), jnp.float32)
        step = 256
        for k in range(0, sample_rows, step):
            x = geno[j, k : k + step, :].astype(jnp.float32)
            squares = squares + jnp.sum((x * x).reshape(step // 8, 8, share), axis=0)
            acc = acc + jnp.dot(
                res_ref[:, k : k + step], x.astype(jnp.bfloat16),
                preferred_element_type=jnp.float32,
            )
        counts = jnp.sum(squares, axis=0, keepdims=True)
        rows = share // LANES
        kind = jnp.concatenate(
            [class_ref[pl.ds(owners[j] * rows + i, 1), :] for i in range(rows)], axis=1
        )
        weight = jnp.zeros((1, share), jnp.float32)
        for c in range(cw_ref.shape[0]):
            weight = jnp.where(kind == c, cw_ref[c], weight)
        scores[j, :phenos, :] = acc * (weight * total_samples ** (-0.5))
        quad = weight * weight * counts / total_samples
        first = lax.broadcasted_iota(jnp.int32, (depth - phenos, share), 0) == 0
        scores[j, phenos:, :] = jnp.where(first, quad, 0.0)

    def rs_copy(r):
        return remote(
            scores.at[r, pl.ds(0, phenos)], partials.at[r], rs_send.at[r], rs_recv.at[r],
            (g, peers[2]),
        )

    for copy in smalls:
        copy.wait()
    chunk(0)
    chunk(1)
    chunk(2)
    chunk(3)

    chunk_sums = [jnp.sum(scores[j], axis=1, keepdims=True) for j in range(GROUPS)]
    wide = lax.broadcasted_iota(jnp.int32, (LANES, LANES), 1)

    def tall(column):
        fill = jnp.zeros((LANES - column.shape[0], 1), jnp.float32)
        return jnp.concatenate([column, fill], axis=0)

    squared = jnp.square(res_ref[...].astype(jnp.float32))
    columns = [jnp.sum(squared, axis=1, keepdims=True)]
    for k in range(GROUPS + 1):
        total = jnp.zeros((depth, 1), jnp.float32)
        for j in range(GROUPS):
            total = total + jnp.where(owners[j] < k, chunk_sums[j], 0.0)
        columns.append(total)
    totals = jnp.zeros((LANES, LANES), jnp.float32)
    for i, column in enumerate(columns):
        totals = jnp.where(wide == i, tall(column), totals)
    totals = jnp.transpose(totals)
    tot_out[...] = totals[GROUPS + 1 : GROUPS + 2]
    pl.semaphore_wait(barrier, genome_count * GROUPS - 1)

    bound_copies = []
    for r in range(3):
        copy = remote(bounds_ref, bounds_in.at[s], bd_send.at[r], bd_recv.at[r], (g, peers[r]))
        copy.start()
        bound_copies.append(copy)
    sends_back = jnp.logical_and(s == 0, g > 0)
    has_next = g < genome_count - 1
    before = lax.rem(g + genome_count - 1, genome_count)
    after = lax.rem(g + 1, genome_count)
    back_copies = [
        remote(bounds_ref, bounds_in.at[GROUPS], bn_send.at[k], bn_recv, (before, k))
        for k in range(GROUPS)
    ]

    @pl.when(sends_back)
    def _():
        for copy in back_copies:
            copy.start()

    rs = [rs_copy(r) for r in (1, 2)]
    for copy in rs:
        copy.start()
    to_copies = []
    for dg in range(1, genome_count):
        for ds in range(GROUPS):
            k = (dg - 1) * GROUPS + ds
            there = (lax.rem(g + dg, genome_count), lax.rem(s + ds, GROUPS))
            to_copies.append(
                (dg, remote(tot_out, tot_in.at[k], to_send.at[k], to_recv.at[k], there))
            )
    for dg in range(genome_count - 1, 0, -1):

        @pl.when(g + dg < genome_count)
        def _(dg=dg):
            for d, copy in to_copies:
                if d == dg:
                    copy.start()

    rs[0].wait()
    relay[...] = scores[0, :phenos, :] + partials[1]
    across = remote(relay, partials.at[0], rs_send.at[0], rs_recv.at[0], (g, peers[0]))
    across.start()
    for copy in bound_copies:
        copy.wait()

    @pl.when(has_next)
    def _():
        back_copies[0].wait_recv()

    lane = lax.broadcasted_iota(jnp.int32, (1, LANES), 1)
    group_of = lane // genes
    start_row = jnp.zeros((1, LANES), jnp.int32)

    def tiled(row):
        return jnp.concatenate([row] * (LANES // genes), axis=1)

    own_bounds = (tiled(bounds_ref[0]), tiled(bounds_ref[1]))
    end_row = jnp.zeros((1, LANES), jnp.int32)
    base = g * block
    for k in range(GROUPS + 1):
        if k < GROUPS:
            use = group_of == k
            lows = jnp.where(s == k, own_bounds[0], tiled(bounds_in[k, 0]))
            tops = jnp.where(s == k, own_bounds[1], tiled(bounds_in[k, 1]))
        else:
            use = jnp.logical_and(group_of == k, has_next)
            lows = tiled(bounds_in[k, 0])
            tops = tiled(bounds_in[k, 1])
        start_row = jnp.where(use, lows - base, start_row)
        end_row = jnp.where(use, tops - base, end_row)

    sums = jnp.zeros((depth, LANES), jnp.float32)
    for j in range(GROUPS):
        v = lax.broadcasted_iota(jnp.int32, (share, LANES), 0) + owners[j] * share
        inside = jnp.logical_and(v >= start_row, v < end_row)
        picker = jnp.where(inside, 1.0, 0.0).astype(jnp.bfloat16)
        sums = sums + dot3(scores[j], picker)
    table = jnp.transpose(
        jnp.concatenate([sums, jnp.zeros((LANES - depth, LANES), jnp.float32)], axis=0)
    )
    for k in range(GROUPS + 1):
        gene_out[k, :genes, :] = table[k * genes : (k + 1) * genes]
        row = lax.broadcasted_iota(jnp.int32, (8, LANES), 0)
        gene_out[k, genes:, :] = jnp.where(
            row == 0, totals[:1], jnp.where(row == 1, totals[1 + k : 2 + k], 0.0)
        )
    ge_copies = []
    for r in range(3):
        copy = remote(
            gene_out.at[peers[r]], gene_in.at[r], ge_send.at[r], ge_recv.at[r], (g, peers[r])
        )
        copy.start()
        ge_copies.append(copy)
    next_copy = remote(
        gene_out.at[GROUPS], gene_in.at[3 + s], gn_send, gn_recv.at[s], (after, 0)
    )

    @pl.when(has_next)
    def _():
        next_copy.start()

    row_u = lax.broadcasted_iota(jnp.int32, (share, share), 0)
    col_v = lax.broadcasted_iota(jnp.int32, (share, share), 1)
    upper = jnp.where(row_u <= col_v, 1.0, 0.0).astype(jnp.bfloat16)
    rs[1].wait()
    across.wait()
    summed = (scores[3, :phenos, :] + partials[2]) + partials[0]
    prefix = dot3(summed, upper)

    for copy in ge_copies:
        copy.wait()
    mine = (gene_out[s] + gene_in[2]) + (gene_in[0] + gene_in[1])
    for k in range(GROUPS):
        arrival = remote(
            gene_out.at[GROUPS], gene_in.at[3 + k], gn_send, gn_recv.at[k], (before, k)
        )
        pl.when(sends_back)(arrival.wait_recv)
    extra = (gene_in[3] + gene_in[4]) + (gene_in[5] + gene_in[6])
    gene_rows = mine[:genes] + jnp.where(sends_back, extra[:genes], 0.0)
    variance = mine[genes : genes + 1, :phenos] / total_samples + 1e-05
    quad = gene_rows[:, phenos : phenos + 1]
    stat_ref[...] = jnp.square(gene_rows[:, :phenos]) / (variance * (quad + 1.0))

    carry = mine[genes + 1 : genes + 2]
    for dg in range(1, genome_count):

        @pl.when(g - dg >= 0)
        def _(dg=dg):
            for d, copy in to_copies:
                if d == dg:
                    copy.wait_recv()

        k = (dg - 1) * GROUPS
        four = (tot_in[k] + tot_in[k + 1]) + (tot_in[k + 2] + tot_in[k + 3])
        carry = carry + jnp.where(g - dg >= 0, four, 0.0)
    column = jnp.transpose(jnp.broadcast_to(carry, (LANES, LANES)))[:phenos]
    for k in range(0, share, LANES):
        track_ref[:, k : k + LANES] = prefix[:, k : k + LANES] + column

    for dg in range(1, genome_count):

        @pl.when(g + dg < genome_count)
        def _(dg=dg):
            for d, copy in to_copies:
                if d == dg:
                    copy.wait_send()

    pl.when(has_next)(next_copy.wait_send)

    @pl.when(sends_back)
    def _():
        for copy in back_copies:
            copy.wait_send()


def finish(scale, track_in, stat_in, track_out, stat_out):
    track_out[...] = track_in[...] * scale
    stat_out[...] = stat_in[...]


def local_kernel(genotypes, residuals, variant_class, class_weight, gene_start, gene_end):
    genome_count = lax.axis_size("genome")
    sample_rows, block_vars = genotypes.shape
    phenos = residuals.shape[1]
    share = block_vars // GROUPS
    genes = gene_start.shape[0]
    depth = phenos + 16
    far = (genome_count - 1) * GROUPS
    vmem = pl.BlockSpec(memory_space=pltpu.VMEM)
    dma = pltpu.SemaphoreType.DMA
    track, stat = pl.pallas_call(
        functools.partial(kernel, genome_count),
        out_shape=(
            pltpu.VMEM((phenos, share), jnp.float32),
            pltpu.VMEM((genes, phenos), jnp.float32),
        ),
        in_specs=[pl.BlockSpec(memory_space=pltpu.HBM)] * 6,
        out_specs=(vmem, vmem),
        scratch_shapes=[
            pltpu.VMEM((phenos, sample_rows), jnp.bfloat16),
            pltpu.VMEM((block_vars // LANES, LANES), jnp.int32),
            pltpu.SMEM(class_weight.shape, jnp.float32),
            pltpu.VMEM((2, 1, genes), jnp.int32),
            dma((5,)),
            pltpu.VMEM((GROUPS, sample_rows, share), jnp.int32),
            pltpu.VMEM((GROUPS, depth, share), jnp.float32),
            pltpu.VMEM((phenos, share), jnp.float32),
            pltpu.VMEM((3, phenos, share), jnp.float32),
            pltpu.VMEM((GROUPS + 1, 2, 1, genes), jnp.int32),
            pltpu.VMEM((GROUPS + 1, genes + 8, LANES), jnp.float32),
            pltpu.VMEM((3 + GROUPS, genes + 8, LANES), jnp.float32),
            pltpu.VMEM((1, LANES), jnp.float32),
            pltpu.VMEM((far, 1, LANES), jnp.float32),
            dma((GROUPS,)), dma((3,)), dma((3,)), dma((3,)), dma((3,)), dma((GROUPS,)), dma(()),
            dma((3,)), dma((3,)), dma(()), dma((GROUPS,)), dma((far,)), dma((far,)),
        ],
        compiler_params=pltpu.CompilerParams(
            collective_id=0, has_side_effects=True, vmem_limit_bytes=VMEM_LIMIT
        ),
    )(*(
        pltpu.with_memory_space_constraint(a, pltpu.HBM)
        for a in (
            genotypes, residuals.T, variant_class.reshape(block_vars // LANES, LANES), class_weight,
            gene_start.reshape(1, genes), gene_end.reshape(1, genes),
        )
    ))
    scale = (block_vars * genome_count) ** (-0.5)
    track, stat = pl.pallas_call(
        functools.partial(finish, scale),
        out_shape=(
            jax.ShapeDtypeStruct((phenos, share), jnp.float32),
            jax.ShapeDtypeStruct((genes, phenos), jnp.float32),
        ),
        in_specs=[vmem, vmem],
        out_specs=(vmem, vmem),
    )(
        pltpu.with_memory_space_constraint(track, pltpu.VMEM),
        pltpu.with_memory_space_constraint(stat, pltpu.VMEM),
    )
    return track.T, stat


def solution(mesh):
    groups = mesh.shape["samples"]

    def body(genotypes, residuals, variant_class, class_weight, gene_start, gene_end):
        args = (genotypes, residuals, variant_class, class_weight, gene_start, gene_end)
        share = genotypes.shape[1] // groups
        genes = gene_start.shape[0]
        fits = LANES % genes == 0 and (GROUPS + 1) * genes <= LANES
        aligned = share % LANES == 0 and genotypes.shape[0] % 256 == 0 and genes % 8 == 0
        if groups == GROUPS and fits and aligned:
            return local_kernel(*args)
        return local(*args)

    return jax.shard_map(
        body,
        mesh=mesh,
        in_specs=(
            P("samples", "genome"),
            P("samples", None),
            P("genome"),
            P(),
            P(("genome", "samples")),
            P(("genome", "samples")),
        ),
        out_specs=(P(("genome", "samples"), None), P(("genome", "samples"), None)),
        check_vma=False,
    )
```
